32 devices in a mesh: batch: 1 (over z), dap: 32 (over y, x, core).
Axes of the slice: x: 4, y: 4, z: 1, core: 2. Of those that a mesh axis runs over, the one named last changes fastest.
The devices are a block of a 4x4x8 slice.
Arguments:
- z_pair: bfloat16 [512, 512, 128], P(('batch', 'dap'))
- msa_feat: bfloat16 [512, 512, 64], P(None, ('batch', 'dap'))
- ln_scale: bfloat16 [64], replicated
- ln_offset: bfloat16 [64], replicated
- w_a: bfloat16 [64, 32], replicated
- b_a: bfloat16 [32], replicated
- w_b: bfloat16 [64, 32], replicated
- b_b: bfloat16 [32], replicated
- w_out: bfloat16 [1024, 128], replicated
- b_out: bfloat16 [128], replicated
Outputs:
- output: bfloat16 [512, 512, 128], P(('batch', 'dap'))
All inputs are finite; a program needn't handle non-finite values.
Results may differ from the reference program's by a relative error of at most 0.001.
Values are sent between devices in bfloat16 or wider.
A program may use at most 768 MiB of HBM per device.

```python
import jax
import jax.numpy as jnp
from jax import lax

MSA_ROWS = 512
N_RES = 512
MSA_DIM = 64
HID_DIM = 32
PAIR_DIM = 128
LOW_RANK = 4

LN_EPS = 1e-5
ROW_TILE = min(N_RES, max(1, 8192 // N_RES))


def normal_draw(rng_key, shape_in, scale_in):
    return jax.random.normal(rng_key, shape_in, jnp.float32) * scale_in


def setup_inputs(seed: int = 0, part: int = 0) -> dict:
    part_keys = jax.random.split(jax.random.fold_in(jax.random.key(seed), part), 4)
    shared_keys = jax.random.split(jax.random.key(seed + 1), 8)
    mix_coef = normal_draw(part_keys[0], (MSA_ROWS, LOW_RANK), 1.0)
    res_feat = normal_draw(part_keys[1], (LOW_RANK, N_RES, MSA_DIM), 1.0)
    msa_noise = normal_draw(part_keys[2], (MSA_ROWS, N_RES, MSA_DIM), 0.5)
    msa_f32 = jnp.einsum('sr,rnm->snm', mix_coef, res_feat) * LOW_RANK ** -0.5 + msa_noise
    z_f32 = normal_draw(part_keys[3], (N_RES, N_RES, PAIR_DIM), 1.0)
    return {
        'z_pair': z_f32.astype(jnp.bfloat16),
        'msa_feat': msa_f32.astype(jnp.bfloat16),
        'ln_scale': (1.0 + normal_draw(shared_keys[0], (MSA_DIM,), 0.5)).astype(jnp.bfloat16),
        'ln_offset': normal_draw(shared_keys[1], (MSA_DIM,), 0.5).astype(jnp.bfloat16),
        'w_a': normal_draw(shared_keys[2], (MSA_DIM, HID_DIM), MSA_DIM ** -0.5).astype(jnp.bfloat16),
        'b_a': normal_draw(shared_keys[3], (HID_DIM,), 0.5).astype(jnp.bfloat16),
        'w_b': normal_draw(shared_keys[4], (MSA_DIM, HID_DIM), MSA_DIM ** -0.5).astype(jnp.bfloat16),
        'b_b': normal_draw(shared_keys[5], (HID_DIM,), 0.5).astype(jnp.bfloat16),
        'w_out': normal_draw(shared_keys[6], (HID_DIM * HID_DIM, PAIR_DIM), (HID_DIM * HID_DIM) ** -0.5).astype(jnp.bfloat16),
        'b_out': normal_draw(shared_keys[7], (PAIR_DIM,), 0.5).astype(jnp.bfloat16),
    }


def layer_norm(msa_feat, ln_scale, ln_offset):
    msa_f32 = msa_feat.astype(jnp.float32)
    mean_val = jnp.mean(msa_f32, axis=-1, keepdims=True)
    centred = msa_f32 - mean_val
    var_val = jnp.mean(centred * centred, axis=-1, keepdims=True)
    normed = centred / jnp.sqrt(var_val + LN_EPS)
    return (normed * ln_scale.astype(jnp.float32) + ln_offset.astype(jnp.float32)).astype(jnp.bfloat16)


def project(msa_norm, weight, bias_vec):
    flat_rows = msa_norm.reshape(-1, msa_norm.shape[-1])
    out_f32 = jnp.dot(flat_rows, weight, preferred_element_type=jnp.float32) + bias_vec.astype(jnp.float32)
    return out_f32.astype(jnp.bfloat16).reshape(msa_norm.shape[0], msa_norm.shape[1], weight.shape[1])


def reference(z_pair, msa_feat, ln_scale, ln_offset, w_a, b_a, w_b, b_b, w_out, b_out):
    msa_norm = layer_norm(msa_feat, ln_scale, ln_offset)
    proj_a = project(msa_norm, w_a, b_a).astype(jnp.float32)
    proj_b = project(msa_norm, w_b, b_b).astype(jnp.float32)
    w_cube = w_out.astype(jnp.float32).reshape(HID_DIM, HID_DIM, PAIR_DIM)
    bias_out = b_out.astype(jnp.float32)
    inv_seq = 1.0 / MSA_ROWS

    def tile_fn(tile_idx):
        row_start = tile_idx * ROW_TILE
        a_tile = lax.dynamic_slice_in_dim(proj_a, row_start, ROW_TILE, axis=1)
        z_tile = lax.dynamic_slice_in_dim(z_pair, row_start, ROW_TILE, axis=0)
        outer_prod = jnp.einsum('sic,sjd->icjd', a_tile, proj_b) * inv_seq
        outer_prod = outer_prod.astype(jnp.bfloat16).astype(jnp.float32)
        update = jnp.einsum('icjd,cdz->ijz', outer_prod, w_cube) + bias_out
        return (z_tile.astype(jnp.float32) + update).astype(jnp.bfloat16)

    row_tiles = lax.map(tile_fn, jnp.arange(N_RES // ROW_TILE))
    return row_tiles.reshape(N_RES, N_RES, PAIR_DIM)
```

```python
import functools
import math

import jax
import jax.numpy as jnp
from jax import lax
from jax.experimental import pallas as pl
from jax.experimental.pallas import tpu as pltpu
from jax.sharding import PartitionSpec as P

LN_EPS = 1e-5
CORES = 2
PARTS = 4
PARTNER_LAG = 3
MESH = pl.DeviceIdType.MESH
F32 = jnp.float32
BF16 = jnp.bfloat16


def forwards(block, part, side):
    first, second = block
    low = part < PARTS // 2
    hops = []
    if second == 0:
        if first == 0 or (first == side - 1 and low):
            hops.append(("A+", ((first - 1) % side, second)))
        if first == 0 or (first == 1 and not low):
            hops.append(("A-", ((first + 1) % side, second)))
        hops.append(("B+", (first, side - 1)))
        hops.append(("B-", (first, 1)))
    elif second == side - 1 and low:
        hops.append(("B+", (first, (second - 1) % side)))
    elif second == 1 and not low:
        hops.append(("B-", (first, (second + 1) % side)))
    return hops


def arrival_order(side):
    queues = {d: [] for d in ("A+", "A-", "B+", "B-")}
    for part in range(PARTS):
        for d, name in forwards((0, 0), part, side):
            queues[d].append((name, part))
    order, turn = [], {"+": 0, "-": 0}
    pending = []
    while any(queues.values()) or pending:
        for name, part in pending:
            order.append((name, part))
            for d, there in forwards(name, part, side):
                queues[d].append((there, part))
        pending = []
        for sign in "+-":
            pick = "AB"[turn[sign]] + sign
            if not queues[pick]:
                pick = "BA"[turn[sign]] + sign
            if queues[pick]:
                pending.append(queues[pick].pop(0))
            turn[sign] = 1 - turn[sign]
    return order


def plan(side):
    own, other = "own", "other"
    units = [(own, (0, 0)), (other, (0, 0))]
    before = [[], []]
    backlog, count, waiting = [], {}, []
    for index, (name, part) in enumerate(arrival_order(side)):
        waiting.append((name, part))
        count[name] = count.get(name, 0) + 1
        if count[name] == PARTS:
            backlog.append((index, own, name))
            backlog.append((index + PARTNER_LAG, other, name))
            backlog.sort(key=lambda item: item[0])
        if backlog and backlog[0][0] <= index:
            _, kind, done = backlog.pop(0)
            units.append((kind, done))
            before.append(waiting)
            waiting = []
    for _, kind, done in backlog:
        units.append((kind, done))
        before.append(waiting)
        waiting = []
    return units, before


def column(row, size):
    shape = (size, size)
    eye = lax.broadcasted_iota(jnp.int32, shape, 0) == lax.broadcasted_iota(jnp.int32, shape, 1)
    return jnp.sum(jnp.where(eye, jnp.broadcast_to(row, shape), 0.0), axis=1, keepdims=True)


def dispatch(index, low, high, actions):
    if not any(actions[low:high]):
        return
    if high - low == 1:
        for action in actions[low]:
            action()
        return
    mid = (low + high) // 2
    if any(actions[low:mid]):
        pl.when(index < mid)(lambda: dispatch(index, low, mid, actions))
    if any(actions[mid:high]):
        pl.when(index >= mid)(lambda: dispatch(index, mid, high, actions))


def kernel(side, units, before, z_hbm, m_hbm, scale_hbm, offset_hbm, wa_hbm, ba_hbm, wb_hbm, bb_hbm, wo_hbm, bo_hbm, out_ref,
           m_ref, scale_ref, offset_ref, wa_ref, ba_ref, wb_ref, bb_ref, wo_ref, bo_ref, z_ref,
           held, a_rows, a_cols, outer, lhs, upd, in_sem, m_sem, wo_sem, z_sem, send_sem, part_sem, block_sem):
    n_loc, msa_dim, n_seq = m_ref.shape
    hid = wa_ref.shape[0]
    rows = n_loc * hid
    part_rows = rows // PARTS
    part_res = n_loc // PARTS
    lanes = 128
    n_hi = rows // lanes
    n_lo = hid // n_hi

    me = lax.axis_index("dap")
    core = lax.rem(me, CORES)
    chip = me // CORES
    x, y = lax.rem(chip, side), chip // side
    pos_a = x * (1 - core) + y * core
    pos_b = y * (1 - core) + x * core

    def device(a, b, which):
        a, b = lax.rem(a, side), lax.rem(b, side)
        return ((b * (1 - core) + a * core) * side + a * (1 - core) + b * core) * CORES + which

    peers = {
        "A+": device(pos_a + 1, pos_b, core),
        "A-": device(pos_a + side - 1, pos_b, core),
        "B+": device(pos_a, pos_b + 1, core),
        "B-": device(pos_a, pos_b + side - 1, core),
        "D": device(pos_a, pos_b, 1 - core),
    }
    lane_of = {d: k for k, d in enumerate(peers)}
    slot = {unit: k for k, unit in enumerate(units)}
    part_index = {}
    for events in before:
        for event in events:
            part_index[event] = len(part_index)
    other_index = {name: k for k, name in enumerate(u[1] for u in units if u[0] == "other")}

    barrier = pltpu.get_barrier_semaphore()
    for peer in peers.values():
        pl.semaphore_signal(barrier, inc=1, device_id={"dap": peer}, device_id_type=MESH)

    m_copies = []
    for g in range(PARTS):
        span = pl.ds(g * part_res, part_res)
        m_copies.append(pltpu.make_async_copy(m_hbm.at[span], m_ref.at[span], m_sem.at[g]))
    small = [pltpu.make_async_copy(s, d, in_sem.at[k]) for k, (s, d) in enumerate((
        (scale_hbm, scale_ref), (offset_hbm, offset_ref), (wa_hbm, wa_ref), (ba_hbm, ba_ref), (wb_hbm, wb_ref),
        (bb_hbm, bb_ref), (bo_hbm, bo_ref)))]
    wo_copies = [pltpu.make_async_copy(wo_hbm.at[:, k], wo_ref.at[k], wo_sem.at[k]) for k in range(n_lo)]
    z_copy = pltpu.make_async_copy(z_hbm, z_ref, z_sem)
    for copy in m_copies[:1] + small + m_copies[1:] + wo_copies + [z_copy]:
        copy.start()

    sent = {d: 0 for d in peers}

    def send(direction, name_here, part, name_there):
        kind_there = "other" if direction == "D" else "own"
        src = slot["own", name_here] * rows + part * part_rows
        dst = slot[kind_there, name_there] * rows + part * part_rows
        sem = block_sem.at[other_index[name_there]] if direction == "D" else part_sem.at[part_index[name_there, part]]
        pltpu.make_async_remote_copy(
            src_ref=held.at[pl.ds(src, part_rows)],
            dst_ref=held.at[pl.ds(dst, part_rows)],
            send_sem=send_sem.at[lane_of[direction]],
            recv_sem=sem,
            device_id={"dap": peers[direction]},
            device_id_type=MESH,
        ).start()

    def pass_on(name, part):
        for direction, there in forwards(name, part, side):
            sent[direction] += 1
            send(direction, name, part, there)
        sent["D"] += 1
        send("D", name, part, name)

    def landed(ref, sem):
        pltpu.make_async_copy(ref, ref, sem).wait()

    def receive(name, part):
        start = slot["own", name] * rows + part * part_rows
        landed(held.at[pl.ds(start, part_rows)], part_sem.at[part_index[name, part]])
        pass_on(name, part)

    def receive_other(name):
        landed(held.at[pl.ds(slot["other", name] * rows, rows)], block_sem.at[other_index[name]])

    for copy in small:
        copy.wait()
    scale = column(scale_ref[...].astype(F32), msa_dim)
    offset = column(offset_ref[...].astype(F32), msa_dim)
    bias = jnp.concatenate([column(ba_ref[...].astype(F32), hid), column(bb_ref[...].astype(F32), hid)], axis=0)
    w_ab = jnp.concatenate([wa_ref[...], wb_ref[...]], axis=0)
    for g in range(PARTS):
        m_copies[g].wait()
        for r in range(g * part_res, (g + 1) * part_res):
            value = m_ref[r].astype(F32)
            mean = jnp.sum(value, axis=0, keepdims=True) * (1.0 / msa_dim)
            centred = value - mean
            var = jnp.sum(centred * centred, axis=0, keepdims=True) * (1.0 / msa_dim)
            normed = centred * lax.rsqrt(var + LN_EPS)
            normed = (normed * scale + offset).astype(BF16)
            both = jnp.dot(w_ab, normed, preferred_element_type=F32) + bias
            for c in range(0, hid, 8):
                for t in range(n_seq // lanes):
                    a_rows[t, pl.ds(c * n_loc + r, 8, stride=n_loc), :] = both[c:c + 8, t * lanes:(t + 1) * lanes]
            held[r * hid:(r + 1) * hid, :] = both[hid:].astype(BF16)
        if g == 0:
            pl.semaphore_wait(barrier, len(peers))
        else:
            pass_on((0, 0), g - 1)
    for t in range(n_seq // lanes):
        a_cols[t * lanes:(t + 1) * lanes, :] = a_rows[t].astype(BF16).T
    pass_on((0, 0), PARTS - 1)

    for copy in wo_copies:
        copy.wait()
    z_copy.wait()

    def out_start(kind, name):
        if kind == "own":
            owner = device(pos_a + name[0], pos_b + name[1], core)
        else:
            owner = device(pos_a + name[1], pos_b + name[0], 1 - core)
        return owner * n_loc

    starts = [out_start(*unit) for unit in units]
    actions = []
    for unit, events in zip(units, before):
        todo = [functools.partial(receive, *event) for event in events]
        if unit[0] == "other":
            todo.append(functools.partial(receive_other, unit[1]))
        actions.append(todo)

    inv_seq = 1.0 / n_seq
    bias_out = bo_ref[...].astype(F32)

    def step(index, carry):
        dispatch(index, 0, len(units), actions)
        start = starts[0]
        for k in range(1, len(units)):
            start = jnp.where(index == k, starts[k], start)
        here = pl.ds(pl.multiple_of(index * rows, rows), rows)
        for c in range(0, rows, 2 * lanes):
            prod = jnp.dot(held[here, :], a_cols[:, c:c + 2 * lanes], preferred_element_type=F32)
            outer[:, c:c + 2 * lanes] = (prod * inv_seq).astype(BF16)
        for j in range(n_loc):
            tile = jnp.concatenate([outer[j * hid:(j + 1) * hid, t * lanes:(t + 1) * lanes] for t in range(n_hi)], axis=0)
            turned = tile.T
            for k in range(n_lo):
                lhs[j * n_loc:(j + 1) * n_loc, k * lanes:(k + 1) * lanes] = turned[k * n_loc:(k + 1) * n_loc]
        w_all = wo_ref[...].reshape(n_lo * n_hi * hid, wo_ref.shape[-1])
        update = jnp.dot(lhs[...], w_all, preferred_element_type=F32) + bias_out
        for j in range(n_loc):
            for i in range(0, n_loc, 8):
                upd[pl.ds(i * n_loc + j, 8, stride=n_loc), :] = update[j * n_loc + i:j * n_loc + i + 8]
        cols = pl.ds(pl.multiple_of(start, n_loc), n_loc)
        total = z_ref[:, cols, :].astype(F32) + upd[...].reshape(n_loc, n_loc, upd.shape[-1])
        out_ref[:, cols, :] = total.astype(BF16)
        return carry

    lax.fori_loop(0, len(units), step, 0)

    for direction in peers:
        landed(held.at[pl.ds(0, sent[direction] * part_rows)], send_sem.at[lane_of[direction]])


def solution(mesh):
    row_spec = P(('batch', 'dap'))
    col_spec = P(None, ('batch', 'dap'))
    rep_spec = P()
    side = math.isqrt(mesh.shape['dap'] // CORES)
    units, before = plan(side)

    def local_update(z_rows, msa, ln_scale, ln_offset, w_a, b_a, w_b, b_b, w_out, b_out):
        n_seq, n_loc, msa_dim = msa.shape
        hid = w_a.shape[1]
        rows = n_loc * hid
        pair_dim = z_rows.shape[2]
        n_hi = rows // 128
        n_lo = hid // n_hi
        n_events = sum(len(events) for events in before)
        n_other = sum(unit[0] == "other" for unit in units)
        row = lambda v: v.reshape(1, -1)
        any_spec = pl.BlockSpec(memory_space=pl.ANY)
        vmem_spec = pl.BlockSpec(memory_space=pltpu.VMEM)
        call = pl.pallas_call(
            functools.partial(kernel, side, units, before),
            out_shape=jax.ShapeDtypeStruct(z_rows.shape, z_rows.dtype),
            in_specs=[any_spec] * 10,
            out_specs=vmem_spec,
            scratch_shapes=[
                pltpu.VMEM((n_loc, msa_dim, n_seq), BF16),
                pltpu.VMEM((1, msa_dim), BF16),
                pltpu.VMEM((1, msa_dim), BF16),
                pltpu.VMEM((hid, msa_dim), BF16),
                pltpu.VMEM((1, hid), BF16),
                pltpu.VMEM((hid, msa_dim), BF16),
                pltpu.VMEM((1, hid), BF16),
                pltpu.VMEM((n_lo, n_hi, hid, pair_dim), BF16),
                pltpu.VMEM((1, pair_dim), BF16),
                pltpu.VMEM(z_rows.shape, BF16),
                pltpu.VMEM((len(units) * rows, n_seq), BF16),
                pltpu.VMEM((n_seq // 128, rows, 128), F32),
                pltpu.VMEM((n_seq, rows), BF16),
                pltpu.VMEM((rows, rows), BF16),
                pltpu.VMEM((n_loc * n_loc, hid * hid), BF16),
                pltpu.VMEM((n_loc * n_loc, pair_dim), F32),
                pltpu.SemaphoreType.DMA((7,)),
                pltpu.SemaphoreType.DMA((PARTS,)),
                pltpu.SemaphoreType.DMA((n_lo,)),
                pltpu.SemaphoreType.DMA,
                pltpu.SemaphoreType.DMA((5,)),
                pltpu.SemaphoreType.DMA((n_events,)),
                pltpu.SemaphoreType.DMA((n_other,)),
            ],
            compiler_params=pltpu.CompilerParams(
                collective_id=0, has_side_effects=True, vmem_limit_bytes=56 * 1024 * 1024),
            name="outer_product_mean",
        )
        return call(z_rows, msa.transpose(1, 2, 0), row(ln_scale), row(ln_offset), w_a.T, row(b_a), w_b.T, row(b_b),
                    w_out.reshape(n_hi, n_lo, hid, pair_dim), row(b_out))

    return jax.shard_map(local_update, mesh=mesh, in_specs=(row_spec, col_spec) + (rep_spec,) * 8, out_specs=row_spec, check_vma=False)
```

```python
import functools
import math

import jax
import jax.numpy as jnp
from jax import lax
from jax.experimental import pallas as pl
from jax.experimental.pallas import tpu as pltpu
from jax.sharding import PartitionSpec as P

LN_EPS = 1e-5
CORES = 2
PARTS = 4
PARTNER_LAG = 3
MESH = pl.DeviceIdType.MESH
F32 = jnp.float32
BF16 = jnp.bfloat16


def forwards(block, part, side):
    first, second = block
    low = part < PARTS // 2
    hops = []
    if second == 0:
        if first == 0 or (first == side - 1 and low):
            hops.append(("A+", ((first - 1) % side, second)))
        if first == 0 or (first == 1 and not low):
            hops.append(("A-", ((first + 1) % side, second)))
        hops.append(("B+", (first, side - 1)))
        hops.append(("B-", (first, 1)))
    elif second == side - 1 and low:
        hops.append(("B+", (first, (second - 1) % side)))
    elif second == 1 and not low:
        hops.append(("B-", (first, (second + 1) % side)))
    return hops


def arrival_order(side):
    queues = {d: [] for d in ("A+", "A-", "B+", "B-")}
    for part in range(PARTS):
        for d, name in forwards((0, 0), part, side):
            queues[d].append((name, part))
    order, turn = [], {"+": 0, "-": 0}
    pending = []
    while any(queues.values()) or pending:
        for name, part in pending:
            order.append((name, part))
            for d, there in forwards(name, part, side):
                queues[d].append((there, part))
        pending = []
        for sign in "+-":
            pick = "AB"[turn[sign]] + sign
            if not queues[pick]:
                pick = "BA"[turn[sign]] + sign
            if queues[pick]:
                pending.append(queues[pick].pop(0))
            turn[sign] = 1 - turn[sign]
    return order


def plan(side):
    own, other = "own", "other"
    units = [(own, (0, 0)), (other, (0, 0))]
    before = [[], []]
    backlog, count, waiting = [], {}, []
    for index, (name, part) in enumerate(arrival_order(side)):
        waiting.append((name, part))
        count[name] = count.get(name, 0) + 1
        if count[name] == PARTS:
            backlog.append((index, own, name))
            backlog.append((index + PARTNER_LAG, other, name))
            backlog.sort(key=lambda item: item[0])
        if backlog and backlog[0][0] <= index:
            _, kind, done = backlog.pop(0)
            units.append((kind, done))
            before.append(waiting)
            waiting = []
    for _, kind, done in backlog:
        units.append((kind, done))
        before.append(waiting)
        waiting = []
    return units, before


def column(row, size):
    shape = (size, size)
    eye = lax.broadcasted_iota(jnp.int32, shape, 0) == lax.broadcasted_iota(jnp.int32, shape, 1)
    return jnp.sum(jnp.where(eye, jnp.broadcast_to(row, shape), 0.0), axis=1, keepdims=True)


def dispatch(index, low, high, actions):
    if not any(actions[low:high]):
        return
    if high - low == 1:
        for action in actions[low]:
            action()
        return
    mid = (low + high) // 2
    if any(actions[low:mid]):
        pl.when(index < mid)(lambda: dispatch(index, low, mid, actions))
    if any(actions[mid:high]):
        pl.when(index >= mid)(lambda: dispatch(index, mid, high, actions))


def kernel(side, units, before, z_hbm, m_hbm, scale_hbm, offset_hbm, wa_hbm, ba_hbm, wb_hbm, bb_hbm, wo_hbm, bo_hbm, out_ref,
           m_ref, scale_ref, offset_ref, wa_ref, ba_ref, wb_ref, bb_ref, wo_ref, bo_ref, z_ref,
           held, a_rows, a_cols, outer, lhs, upd, in_sem, m_sem, wo_sem, z_sem, send_sem, part_sem, block_sem):
    n_loc, msa_dim, n_seq = m_ref.shape
    hid = wa_ref.shape[0]
    rows = n_loc * hid
    part_rows = rows // PARTS
    part_res = n_loc // PARTS
    lanes = 128
    n_hi = rows // lanes
    n_lo = hid // n_hi

    me = lax.axis_index("dap")
    core = lax.rem(me, CORES)
    chip = me // CORES
    x, y = lax.rem(chip, side), chip // side
    pos_a = x * (1 - core) + y * core
    pos_b = y * (1 - core) + x * core

    def device(a, b, which):
        a, b = lax.rem(a, side), lax.rem(b, side)
        return ((b * (1 - core) + a * core) * side + a * (1 - core) + b * core) * CORES + which

    peers = {
        "A+": device(pos_a + 1, pos_b, core),
        "A-": device(pos_a + side - 1, pos_b, core),
        "B+": device(pos_a, pos_b + 1, core),
        "B-": device(pos_a, pos_b + side - 1, core),
        "D": device(pos_a, pos_b, 1 - core),
    }
    lane_of = {d: k for k, d in enumerate(peers)}
    slot = {unit: k for k, unit in enumerate(units)}
    part_index = {}
    for events in before:
        for event in events:
            part_index[event] = len(part_index)
    other_index = {name: k for k, name in enumerate(u[1] for u in units if u[0] == "other")}

    barrier = pltpu.get_barrier_semaphore()
    for peer in peers.values():
        pl.semaphore_signal(barrier, inc=1, device_id={"dap": peer}, device_id_type=MESH)

    m_copies = []
    for g in range(PARTS):
        span = pl.ds(g * part_res, part_res)
        m_copies.append(pltpu.make_async_copy(m_hbm.at[span], m_ref.at[span], m_sem.at[g]))
    small = [pltpu.make_async_copy(s, d, in_sem.at[k]) for k, (s, d) in enumerate((
        (scale_hbm, scale_ref), (offset_hbm, offset_ref), (wa_hbm, wa_ref), (ba_hbm, ba_ref), (wb_hbm, wb_ref),
        (bb_hbm, bb_ref), (bo_hbm, bo_ref)))]
    wo_copies = [pltpu.make_async_copy(wo_hbm.at[:, k], wo_ref.at[k], wo_sem.at[k]) for k in range(n_lo)]
    z_copy = pltpu.make_async_copy(z_hbm, z_ref, z_sem)
    for copy in m_copies[:1] + small + m_copies[1:] + wo_copies + [z_copy]:
        copy.start()

    sent = {d: 0 for d in peers}

    def send(direction, name_here, part, name_there):
        kind_there = "other" if direction == "D" else "own"
        src = slot["own", name_here] * rows + part * part_rows
        dst = slot[kind_there, name_there] * rows + part * part_rows
        sem = block_sem.at[other_index[name_there]] if direction == "D" else part_sem.at[part_index[name_there, part]]
        pltpu.make_async_remote_copy(
            src_ref=held.at[pl.ds(src, part_rows)],
            dst_ref=held.at[pl.ds(dst, part_rows)],
            send_sem=send_sem.at[lane_of[direction]],
            recv_sem=sem,
            device_id={"dap": peers[direction]},
            device_id_type=MESH,
        ).start()

    def pass_on(name, part):
        for direction, there in forwards(name, part, side):
            sent[direction] += 1
            send(direction, name, part, there)
        sent["D"] += 1
        send("D", name, part, name)

    def landed(ref, sem):
        pltpu.make_async_copy(ref, ref, sem).wait()

    def receive(name, part):
        start = slot["own", name] * rows + part * part_rows
        landed(held.at[pl.ds(start, part_rows)], part_sem.at[part_index[name, part]])
        pass_on(name, part)

    def receive_other(name):
        landed(held.at[pl.ds(slot["other", name] * rows, rows)], block_sem.at[other_index[name]])

    for copy in small:
        copy.wait()
    scale = column(scale_ref[...].astype(F32), msa_dim)
    offset = column(offset_ref[...].astype(F32), msa_dim)
    bias = jnp.concatenate([column(ba_ref[...].astype(F32), hid), column(bb_ref[...].astype(F32), hid)], axis=0)
    w_ab = jnp.concatenate([wa_ref[...], wb_ref[...]], axis=0)
    for g in range(PARTS):
        m_copies[g].wait()
        for r in range(g * part_res, (g + 1) * part_res):
            value = m_ref[r].astype(F32)
            mean = jnp.sum(value, axis=0, keepdims=True) * (1.0 / msa_dim)
            centred = value - mean
            var = jnp.sum(centred * centred, axis=0, keepdims=True) * (1.0 / msa_dim)
            normed = centred * lax.rsqrt(var + LN_EPS)
            normed = (normed * scale + offset).astype(BF16)
            both = jnp.dot(w_ab, normed, preferred_element_type=F32) + bias
            for c in range(0, hid, 8):
                for t in range(n_seq // lanes):
                    a_rows[t, pl.ds(c * n_loc + r, 8, stride=n_loc), :] = both[c:c + 8, t * lanes:(t + 1) * lanes]
            held[r * hid:(r + 1) * hid, :] = both[hid:].astype(BF16)
            if r == part_res:
                pl.semaphore_wait(barrier, len(peers))
            if r and r % part_res == 0:
                pass_on((0, 0), g - 1)
    for t in range(n_seq // lanes):
        a_cols[t * lanes:(t + 1) * lanes, :] = a_rows[t].astype(BF16).T
    pass_on((0, 0), PARTS - 1)

    for copy in wo_copies:
        copy.wait()
    z_copy.wait()

    def out_start(kind, name):
        if kind == "own":
            owner = device(pos_a + name[0], pos_b + name[1], core)
        else:
            owner = device(pos_a + name[1], pos_b + name[0], 1 - core)
        return owner * n_loc

    starts = [out_start(*unit) for unit in units]
    actions = []
    for unit, events in zip(units, before):
        todo = [functools.partial(receive, *event) for event in events]
        if unit[0] == "other":
            todo.append(functools.partial(receive_other, unit[1]))
        actions.append(todo)

    inv_seq = 1.0 / n_seq
    bias_out = bo_ref[...].astype(F32)

    def step(index, carry):
        dispatch(index, 0, len(units), actions)
        start = starts[0]
        for k in range(1, len(units)):
            start = jnp.where(index == k, starts[k], start)
        here = pl.ds(pl.multiple_of(index * rows, rows), rows)
        for c in range(0, rows, 2 * lanes):
            prod = jnp.dot(held[here, :], a_cols[:, c:c + 2 * lanes], preferred_element_type=F32)
            outer[:, c:c + 2 * lanes] = (prod * inv_seq).astype(BF16)
        for j in range(n_loc):
            tile = jnp.concatenate([outer[j * hid:(j + 1) * hid, t * lanes:(t + 1) * lanes] for t in range(n_hi)], axis=0)
            turned = tile.T
            for k in range(n_lo):
                lhs[j * n_loc:(j + 1) * n_loc, k * lanes:(k + 1) * lanes] = turned[k * n_loc:(k + 1) * n_loc]
        w_all = wo_ref[...].reshape(n_lo * n_hi * hid, wo_ref.shape[-1])
        update = jnp.dot(lhs[...], w_all, preferred_element_type=F32) + bias_out
        for j in range(n_loc):
            for i in range(0, n_loc, 8):
                upd[pl.ds(i * n_loc + j, 8, stride=n_loc), :] = update[j * n_loc + i:j * n_loc + i + 8]
        cols = pl.ds(pl.multiple_of(start, n_loc), n_loc)
        total = z_ref[:, cols, :].astype(F32) + upd[...].reshape(n_loc, n_loc, upd.shape[-1])
        out_ref[:, cols, :] = total.astype(BF16)
        return carry

    lax.fori_loop(0, len(units), step, 0)

    for direction in peers:
        landed(held.at[pl.ds(0, sent[direction] * part_rows)], send_sem.at[lane_of[direction]])


def solution(mesh):
    row_spec = P(('batch', 'dap'))
    col_spec = P(None, ('batch', 'dap'))
    rep_spec = P()
    side = math.isqrt(mesh.shape['dap'] // CORES)
    units, before = plan(side)

    def local_update(z_rows, msa, ln_scale, ln_offset, w_a, b_a, w_b, b_b, w_out, b_out):
        n_seq, n_loc, msa_dim = msa.shape
        hid = w_a.shape[1]
        rows = n_loc * hid
        pair_dim = z_rows.shape[2]
        n_hi = rows // 128
        n_lo = hid // n_hi
        n_events = sum(len(events) for events in before)
        n_other = sum(unit[0] == "other" for unit in units)
        row = lambda v: v.reshape(1, -1)
        any_spec = pl.BlockSpec(memory_space=pl.ANY)
        vmem_spec = pl.BlockSpec(memory_space=pltpu.VMEM)
        call = pl.pallas_call(
            functools.partial(kernel, side, units, before),
            out_shape=pltpu.VMEM(z_rows.shape, z_rows.dtype),
            in_specs=[any_spec] * 10,
            out_specs=vmem_spec,
            scratch_shapes=[
                pltpu.VMEM((n_loc, msa_dim, n_seq), BF16),
                pltpu.VMEM((1, msa_dim), BF16),
                pltpu.VMEM((1, msa_dim), BF16),
                pltpu.VMEM((hid, msa_dim), BF16),
                pltpu.VMEM((1, hid), BF16),
                pltpu.VMEM((hid, msa_dim), BF16),
                pltpu.VMEM((1, hid), BF16),
                pltpu.VMEM((n_lo, n_hi, hid, pair_dim), BF16),
                pltpu.VMEM((1, pair_dim), BF16),
                pltpu.VMEM(z_rows.shape, BF16),
                pltpu.VMEM((len(units) * rows, n_seq), BF16),
                pltpu.VMEM((n_seq // 128, rows, 128), F32),
                pltpu.VMEM((n_seq, rows), BF16),
                pltpu.VMEM((rows, rows), BF16),
                pltpu.VMEM((n_loc * n_loc, hid * hid), BF16),
                pltpu.VMEM((n_loc * n_loc, pair_dim), F32),
                pltpu.SemaphoreType.DMA((7,)),
                pltpu.SemaphoreType.DMA((PARTS,)),
                pltpu.SemaphoreType.DMA((n_lo,)),
                pltpu.SemaphoreType.DMA,
                pltpu.SemaphoreType.DMA((5,)),
                pltpu.SemaphoreType.DMA((n_events,)),
                pltpu.SemaphoreType.DMA((n_other,)),
            ],
            compiler_params=pltpu.CompilerParams(
                collective_id=0, has_side_effects=True, vmem_limit_bytes=56 * 1024 * 1024),
            name="outer_product_mean",
        )
        return call(z_rows, msa.transpose(1, 2, 0), row(ln_scale), row(ln_offset), w_a.T, row(b_a), w_b.T, row(b_b),
                    w_out.reshape(n_hi, n_lo, hid, pair_dim), row(b_out))

    return jax.shard_map(local_update, mesh=mesh, in_specs=(row_spec, col_spec) + (rep_spec,) * 8, out_specs=row_spec, check_vma=False)
```

```python
import functools
import math

import jax
import jax.numpy as jnp
from jax import lax
from jax.experimental import pallas as pl
from jax.experimental.pallas import tpu as pltpu
from jax.sharding import PartitionSpec as P

LN_EPS = 1e-5
CORES = 2
PARTS = 8
PARTNER_LAG = 6
MESH = pl.DeviceIdType.MESH
F32 = jnp.float32
BF16 = jnp.bfloat16


def forwards(block, part, side):
    first, second = block
    low = part < PARTS // 2
    hops = []
    if second == 0:
        if first == 0 or (first == side - 1 and low):
            hops.append(("A+", ((first - 1) % side, second)))
        if first == 0 or (first == 1 and not low):
            hops.append(("A-", ((first + 1) % side, second)))
        hops.append(("B+", (first, side - 1)))
        hops.append(("B-", (first, 1)))
    elif second == side - 1 and low:
        hops.append(("B+", (first, (second - 1) % side)))
    elif second == 1 and not low:
        hops.append(("B-", (first, (second + 1) % side)))
    return hops


def arrival_order(side):
    queues = {d: [] for d in ("A+", "A-", "B+", "B-")}
    for part in range(PARTS):
        for d, name in forwards((0, 0), part, side):
            queues[d].append((name, part))
    order, turn = [], {"+": 0, "-": 0}
    pending = []
    while any(queues.values()) or pending:
        for name, part in pending:
            order.append((name, part))
            for d, there in forwards(name, part, side):
                queues[d].append((there, part))
        pending = []
        for sign in "+-":
            pick = "AB"[turn[sign]] + sign
            if not queues[pick]:
                pick = "BA"[turn[sign]] + sign
            if queues[pick]:
                pending.append(queues[pick].pop(0))
            turn[sign] = 1 - turn[sign]
    return order


def plan(side):
    own, other = "own", "other"
    units = [(own, (0, 0)), (other, (0, 0))]
    before = [[], []]
    backlog, count, waiting = [], {}, []
    for index, (name, part) in enumerate(arrival_order(side)):
        waiting.append((name, part))
        count[name] = count.get(name, 0) + 1
        if count[name] == PARTS:
            backlog.append((index, own, name))
            backlog.append((index + PARTNER_LAG, other, name))
            backlog.sort(key=lambda item: item[0])
        if backlog and backlog[0][0] <= index:
            _, kind, done = backlog.pop(0)
            units.append((kind, done))
            before.append(waiting)
            waiting = []
    for _, kind, done in backlog:
        units.append((kind, done))
        before.append(waiting)
        waiting = []
    return units, before


def column(row, size):
    shape = (size, size)
    eye = lax.broadcasted_iota(jnp.int32, shape, 0) == lax.broadcasted_iota(jnp.int32, shape, 1)
    return jnp.sum(jnp.where(eye, jnp.broadcast_to(row, shape), 0.0), axis=1, keepdims=True)


def dispatch(index, low, high, actions):
    if not any(actions[low:high]):
        return
    if high - low == 1:
        for action in actions[low]:
            action()
        return
    mid = (low + high) // 2
    if any(actions[low:mid]):
        pl.when(index < mid)(lambda: dispatch(index, low, mid, actions))
    if any(actions[mid:high]):
        pl.when(index >= mid)(lambda: dispatch(index, mid, high, actions))


def kernel(side, units, before, z_hbm, m_hbm, scale_hbm, offset_hbm, wa_hbm, ba_hbm, wb_hbm, bb_hbm, wo_hbm, bo_hbm, out_ref,
           m_ref, scale_ref, offset_ref, wa_ref, ba_ref, wb_ref, bb_ref, wo_ref, bo_ref, z_ref,
           held, a_rows, a_cols, outer, lhs, upd, in_sem, m_sem, wo_sem, z_sem, send_sem, part_sem, block_sem):
    n_loc, msa_dim, n_seq = m_ref.shape
    hid = wa_ref.shape[0]
    rows = n_loc * hid
    part_rows = rows // PARTS
    part_res = n_loc // PARTS
    lanes = 128
    n_hi = rows // lanes
    n_lo = hid // n_hi

    me = lax.axis_index("dap")
    core = lax.rem(me, CORES)
    chip = me // CORES
    x, y = lax.rem(chip, side), chip // side
    pos_a = x * (1 - core) + y * core
    pos_b = y * (1 - core) + x * core

    def device(a, b, which):
        a, b = lax.rem(a, side), lax.rem(b, side)
        return ((b * (1 - core) + a * core) * side + a * (1 - core) + b * core) * CORES + which

    peers = {
        "A+": device(pos_a + 1, pos_b, core),
        "A-": device(pos_a + side - 1, pos_b, core),
        "B+": device(pos_a, pos_b + 1, core),
        "B-": device(pos_a, pos_b + side - 1, core),
        "D": device(pos_a, pos_b, 1 - core),
    }
    lane_of = {d: k for k, d in enumerate(peers)}
    slot = {unit: k for k, unit in enumerate(units)}
    part_index = {}
    for events in before:
        for event in events:
            part_index[event] = len(part_index)
    other_index = {name: k for k, name in enumerate(u[1] for u in units if u[0] == "other")}

    barrier = pltpu.get_barrier_semaphore()
    for peer in peers.values():
        pl.semaphore_signal(barrier, inc=1, device_id={"dap": peer}, device_id_type=MESH)

    m_copies = []
    for g in range(PARTS):
        span = pl.ds(g * part_res, part_res)
        m_copies.append(pltpu.make_async_copy(m_hbm.at[span], m_ref.at[span], m_sem.at[g]))
    small = [pltpu.make_async_copy(s, d, in_sem.at[k]) for k, (s, d) in enumerate((
        (scale_hbm, scale_ref), (offset_hbm, offset_ref), (wa_hbm, wa_ref), (ba_hbm, ba_ref), (wb_hbm, wb_ref),
        (bb_hbm, bb_ref), (bo_hbm, bo_ref)))]
    wo_copies = [pltpu.make_async_copy(wo_hbm.at[:, k], wo_ref.at[k], wo_sem.at[k]) for k in range(n_lo)]
    z_copy = pltpu.make_async_copy(z_hbm, z_ref, z_sem)
    for copy in m_copies[:1] + small + m_copies[1:] + wo_copies + [z_copy]:
        copy.start()

    sent = {d: 0 for d in peers}

    def send(direction, name_here, part, name_there):
        kind_there = "other" if direction == "D" else "own"
        src = slot["own", name_here] * rows + part * part_rows
        dst = slot[kind_there, name_there] * rows + part * part_rows
        sem = block_sem.at[other_index[name_there]] if direction == "D" else part_sem.at[part_index[name_there, part]]
        pltpu.make_async_remote_copy(
            src_ref=held.at[pl.ds(src, part_rows)],
            dst_ref=held.at[pl.ds(dst, part_rows)],
            send_sem=send_sem.at[lane_of[direction]],
            recv_sem=sem,
            device_id={"dap": peers[direction]},
            device_id_type=MESH,
        ).start()

    def pass_on(name, part):
        for direction, there in forwards(name, part, side):
            sent[direction] += 1
            send(direction, name, part, there)
        sent["D"] += 1
        send("D", name, part, name)

    def landed(ref, sem):
        pltpu.make_async_copy(ref, ref, sem).wait()

    def receive(name, part):
        start = slot["own", name] * rows + part * part_rows
        landed(held.at[pl.ds(start, part_rows)], part_sem.at[part_index[name, part]])
        pass_on(name, part)

    def receive_other(name):
        landed(held.at[pl.ds(slot["other", name] * rows, rows)], block_sem.at[other_index[name]])

    for copy in small:
        copy.wait()
    scale = column(scale_ref[...].astype(F32), msa_dim)
    offset = column(offset_ref[...].astype(F32), msa_dim)
    bias = jnp.concatenate([column(ba_ref[...].astype(F32), hid), column(bb_ref[...].astype(F32), hid)], axis=0)
    w_ab = jnp.concatenate([wa_ref[...], wb_ref[...]], axis=0)
    for g in range(PARTS):
        m_copies[g].wait()
        for r in range(g * part_res, (g + 1) * part_res):
            value = m_ref[r].astype(F32)
            mean = jnp.sum(value, axis=0, keepdims=True) * (1.0 / msa_dim)
            centred = value - mean
            var = jnp.sum(centred * centred, axis=0, keepdims=True) * (1.0 / msa_dim)
            normed = centred * lax.rsqrt(var + LN_EPS)
            normed = (normed * scale + offset).astype(BF16)
            both = jnp.dot(w_ab, normed, preferred_element_type=F32) + bias
            for c in range(0, hid, 8):
                for t in range(n_seq // lanes):
                    a_rows[t, pl.ds(c * n_loc + r, 8, stride=n_loc), :] = both[c:c + 8, t * lanes:(t + 1) * lanes]
            held[r * hid:(r + 1) * hid, :] = both[hid:].astype(BF16)
            if r == part_res:
                pl.semaphore_wait(barrier, len(peers))
            if r and r % part_res == 0:
                pass_on((0, 0), g - 1)
    for t in range(n_seq // lanes):
        a_cols[t * lanes:(t + 1) * lanes, :] = a_rows[t].astype(BF16).T
    pass_on((0, 0), PARTS - 1)

    for copy in wo_copies:
        copy.wait()
    z_copy.wait()

    def out_start(kind, name):
        if kind == "own":
            owner = device(pos_a + name[0], pos_b + name[1], core)
        else:
            owner = device(pos_a + name[1], pos_b + name[0], 1 - core)
        return owner * n_loc

    starts = [out_start(*unit) for unit in units]
    actions = []
    for unit, events in zip(units, before):
        todo = [functools.partial(receive, *event) for event in events]
        if unit[0] == "other":
            todo.append(functools.partial(receive_other, unit[1]))
        actions.append(todo)

    inv_seq = 1.0 / n_seq
    bias_out = bo_ref[...].astype(F32)

    def step(index, carry):
        dispatch(index, 0, len(units), actions)
        start = starts[0]
        for k in range(1, len(units)):
            start = jnp.where(index == k, starts[k], start)
        here = pl.ds(pl.multiple_of(index * rows, rows), rows)
        for c in range(0, rows, 2 * lanes):
            prod = jnp.dot(held[here, :], a_cols[:, c:c + 2 * lanes], preferred_element_type=F32)
            outer[:, c:c + 2 * lanes] = (prod * inv_seq).astype(BF16)
        for j in range(n_loc):
            tile = jnp.concatenate([outer[j * hid:(j + 1) * hid, t * lanes:(t + 1) * lanes] for t in range(n_hi)], axis=0)
            turned = tile.T
            for k in range(n_lo):
                lhs[j * n_loc:(j + 1) * n_loc, k * lanes:(k + 1) * lanes] = turned[k * n_loc:(k + 1) * n_loc]
        w_all = wo_ref[...].reshape(n_lo * n_hi * hid, wo_ref.shape[-1])
        update = jnp.dot(lhs[...], w_all, preferred_element_type=F32) + bias_out
        for j in range(n_loc):
            for i in range(0, n_loc, 8):
                upd[pl.ds(i * n_loc + j, 8, stride=n_loc), :] = update[j * n_loc + i:j * n_loc + i + 8]
        cols = pl.ds(pl.multiple_of(start, n_loc), n_loc)
        total = z_ref[:, cols, :].astype(F32) + upd[...].reshape(n_loc, n_loc, upd.shape[-1])
        out_ref[:, cols, :] = total.astype(BF16)
        return carry

    lax.fori_loop(0, len(units), step, 0)

    for direction in peers:
        landed(held.at[pl.ds(0, sent[direction] * part_rows)], send_sem.at[lane_of[direction]])


def solution(mesh):
    row_spec = P(('batch', 'dap'))
    col_spec = P(None, ('batch', 'dap'))
    rep_spec = P()
    side = math.isqrt(mesh.shape['dap'] // CORES)
    units, before = plan(side)

    def local_update(z_rows, msa, ln_scale, ln_offset, w_a, b_a, w_b, b_b, w_out, b_out):
        n_seq, n_loc, msa_dim = msa.shape
        hid = w_a.shape[1]
        rows = n_loc * hid
        pair_dim = z_rows.shape[2]
        n_hi = rows // 128
        n_lo = hid // n_hi
        n_events = sum(len(events) for events in before)
        n_other = sum(unit[0] == "other" for unit in units)
        row = lambda v: v.reshape(1, -1)
        any_spec = pl.BlockSpec(memory_space=pl.ANY)
        vmem_spec = pl.BlockSpec(memory_space=pltpu.VMEM)
        call = pl.pallas_call(
            functools.partial(kernel, side, units, before),
            out_shape=pltpu.VMEM(z_rows.shape, z_rows.dtype),
            in_specs=[any_spec] * 10,
            out_specs=vmem_spec,
            scratch_shapes=[
                pltpu.VMEM((n_loc, msa_dim, n_seq), BF16),
                pltpu.VMEM((1, msa_dim), BF16),
                pltpu.VMEM((1, msa_dim), BF16),
                pltpu.VMEM((hid, msa_dim), BF16),
                pltpu.VMEM((1, hid), BF16),
                pltpu.VMEM((hid, msa_dim), BF16),
                pltpu.VMEM((1, hid), BF16),
                pltpu.VMEM((n_lo, n_hi, hid, pair_dim), BF16),
                pltpu.VMEM((1, pair_dim), BF16),
                pltpu.VMEM(z_rows.shape, BF16),
                pltpu.VMEM((len(units) * rows, n_seq), BF16),
                pltpu.VMEM((n_seq // 128, rows, 128), F32),
                pltpu.VMEM((n_seq, rows), BF16),
                pltpu.VMEM((rows, rows), BF16),
                pltpu.VMEM((n_loc * n_loc, hid * hid), BF16),
                pltpu.VMEM((n_loc * n_loc, pair_dim), F32),
                pltpu.SemaphoreType.DMA((7,)),
                pltpu.SemaphoreType.DMA((PARTS,)),
                pltpu.SemaphoreType.DMA((n_lo,)),
                pltpu.SemaphoreType.DMA,
                pltpu.SemaphoreType.DMA((5,)),
                pltpu.SemaphoreType.DMA((n_events,)),
                pltpu.SemaphoreType.DMA((n_other,)),
            ],
            compiler_params=pltpu.CompilerParams(
                collective_id=0, has_side_effects=True, vmem_limit_bytes=56 * 1024 * 1024),
            name="outer_product_mean",
        )
        return call(z_rows, msa.transpose(1, 2, 0), row(ln_scale), row(ln_offset), w_a.T, row(b_a), w_b.T, row(b_b),
                    w_out.reshape(n_hi, n_lo, hid, pair_dim), row(b_out))

    return jax.shard_map(local_update, mesh=mesh, in_specs=(row_spec, col_spec) + (rep_spec,) * 8, out_specs=row_spec, check_vma=False)
```

```python
import functools
import heapq
import itertools
import math

import jax
import jax.numpy as jnp
from jax import lax
from jax.experimental import pallas as pl
from jax.experimental.pallas import tpu as pltpu
from jax.sharding import PartitionSpec as P

LN_EPS = 1e-5
CORES = 2
PART_SIZES = (2, 6, 8)
LINK_LATENCY = 5.0
PARTNER_LATENCY = 3.3
UNIT_TIME = 1.9
NORM_TIME = 0.26
MESH = pl.DeviceIdType.MESH
F32 = jnp.float32
BF16 = jnp.bfloat16
OWN = ("mine", 0, 0)


def forwards(name, part, over_link, side):
    kind, along, across = name
    low = sum(PART_SIZES[:part + 1]) * 2 <= sum(PART_SIZES)
    hops = []
    if not over_link and along == 0 and (kind == "other" or across == 0):
        hops.append(("+", (kind, side - 1, across)))
        hops.append(("-", (kind, 1, across)))
    elif over_link and along == side - 1 and low:
        hops.append(("+", (kind, along - 1, across)))
    elif over_link and along == 1 and not low:
        hops.append(("-", (kind, along + 1, across)))
    if over_link or name == OWN:
        hops.append(("core", ("other" if kind == "mine" else "mine", across, along)))
    return hops


def plan(side):
    tick = itertools.count()
    heap, free, events, ready = [], {"+": 0.0, "-": 0.0}, [], {}
    begin = NORM_TIME * sum(PART_SIZES) + UNIT_TIME
    ready[OWN] = begin
    for part in range(len(PART_SIZES)):
        heapq.heappush(heap, (NORM_TIME * sum(PART_SIZES[:part + 1]), next(tick), OWN, part, None))
    while heap:
        time, _, name, part, over_link = heapq.heappop(heap)
        if over_link is not None:
            ready[name] = max(ready.get(name, 0.0), time)
            if over_link or name[0] == "other":
                events.append((time, name, part, over_link))
        for direction, there in forwards(name, part, over_link, side):
            if direction == "core":
                at = time + PARTNER_LATENCY + 0.05 * PART_SIZES[part]
            else:
                free[direction] = max(free[direction], time) + PART_SIZES[part]
                at = free[direction] + LINK_LATENCY
            heapq.heappush(heap, (at, next(tick), there, part, direction != "core"))
    todo = sorted((time, name) for name, time in ready.items())
    units, before, waiting, now = [], [], [], begin
    while todo:
        if events and events[0][0] <= now:
            waiting.append(events.pop(0)[1:])
        elif todo[0][0] <= now:
            units.append(todo.pop(0)[1])
            before.append(waiting)
            waiting = []
            now += UNIT_TIME
        else:
            now = min([todo[0][0]] + [event[0] for event in events[:1]])
    return units, before


def column(row, size):
    shape = (size, size)
    eye = lax.broadcasted_iota(jnp.int32, shape, 0) == lax.broadcasted_iota(jnp.int32, shape, 1)
    return jnp.sum(jnp.where(eye, jnp.broadcast_to(row, shape), 0.0), axis=1, keepdims=True)


def dispatch(index, low, high, actions):
    if not any(actions[low:high]):
        return
    if high - low == 1:
        for action in actions[low]:
            action()
        return
    mid = (low + high) // 2
    if any(actions[low:mid]):
        pl.when(index < mid)(lambda: dispatch(index, low, mid, actions))
    if any(actions[mid:high]):
        pl.when(index >= mid)(lambda: dispatch(index, mid, high, actions))


def kernel(side, units, before, z_hbm, m_hbm, scale_hbm, offset_hbm, wa_hbm, ba_hbm, wb_hbm, bb_hbm, wo_hbm, bo_hbm, out_ref,
           m_ref, scale_ref, offset_ref, wa_ref, ba_ref, wb_ref, bb_ref, wo_ref, bo_ref, z_ref,
           held, a_rows, a_cols, outer, lhs, upd, in_sem, m_sem, wo_sem, z_sem, send_sem, part_sem, block_sem):
    n_loc, msa_dim, n_seq = m_ref.shape
    hid = wa_ref.shape[0]
    rows = n_loc * hid
    ends = list(itertools.accumulate(PART_SIZES))
    begins = [0] + ends[:-1]
    lanes = 128
    n_hi = rows // lanes
    n_lo = hid // n_hi

    me = lax.axis_index("dap")
    core = lax.rem(me, CORES)
    chip = me // CORES
    x, y = lax.rem(chip, side), chip // side
    pos_a = x * (1 - core) + y * core
    pos_b = y * (1 - core) + x * core

    def device(along, across, which):
        a, b = lax.rem(pos_a + along, side), lax.rem(pos_b + across, side)
        return ((b * (1 - core) + a * core) * side + a * (1 - core) + b * core) * CORES + which

    peers = {"+": device(1, 0, core), "-": device(side - 1, 0, core), "core": device(0, 0, 1 - core)}
    lane_of = {d: k for k, d in enumerate(peers)}
    slot = {name: k for k, name in enumerate(units)}
    part_index = {}
    for events in before:
        for name, part, _ in events:
            part_index[name, part] = len(part_index)
    whole = [name for name in units if name != OWN and (name, 0) not in part_index]
    block_index = {name: k for k, name in enumerate(whole)}

    barrier = pltpu.get_barrier_semaphore()
    for peer in peers.values():
        pl.semaphore_signal(barrier, inc=1, device_id={"dap": peer}, device_id_type=MESH)

    m_copies = []
    for k, (lo, hi) in enumerate(zip(begins, ends)):
        m_copies.append(pltpu.make_async_copy(m_hbm.at[lo:hi], m_ref.at[lo:hi], m_sem.at[k]))
    small = [pltpu.make_async_copy(s, d, in_sem.at[k]) for k, (s, d) in enumerate((
        (scale_hbm, scale_ref), (offset_hbm, offset_ref), (wa_hbm, wa_ref), (ba_hbm, ba_ref), (wb_hbm, wb_ref),
        (bb_hbm, bb_ref), (bo_hbm, bo_ref)))]
    wo_copies = [pltpu.make_async_copy(wo_hbm.at[:, k], wo_ref.at[k], wo_sem.at[k]) for k in range(n_lo)]
    z_copy = pltpu.make_async_copy(z_hbm, z_ref, z_sem)
    for copy in m_copies[:1] + small + m_copies[1:] + wo_copies + [z_copy]:
        copy.start()

    sent = {d: 0 for d in peers}

    def span(name, part):
        return pl.ds(slot[name] * rows + begins[part] * hid, PART_SIZES[part] * hid)

    def pass_on(name, part, over_link):
        for direction, there in forwards(name, part, over_link, side):
            sent[direction] += PART_SIZES[part] * hid
            pltpu.make_async_remote_copy(
                src_ref=held.at[span(name, part)],
                dst_ref=held.at[span(there, part)],
                send_sem=send_sem.at[lane_of[direction]],
                recv_sem=block_sem.at[block_index[there]] if there in block_index else part_sem.at[part_index[there, part]],
                device_id={"dap": peers[direction]},
                device_id_type=MESH,
            ).start()

    def landed(ref, sem):
        pltpu.make_async_copy(ref, ref, sem).wait()

    def receive(name, part, over_link):
        landed(held.at[span(name, part)], part_sem.at[part_index[name, part]])
        pass_on(name, part, over_link)

    def receive_block(name):
        landed(held.at[pl.ds(slot[name] * rows, rows)], block_sem.at[block_index[name]])

    for copy in small:
        copy.wait()
    scale = column(scale_ref[...].astype(F32), msa_dim)
    offset = column(offset_ref[...].astype(F32), msa_dim)
    bias = jnp.concatenate([column(ba_ref[...].astype(F32), hid), column(bb_ref[...].astype(F32), hid)], axis=0)
    w_ab = jnp.concatenate([wa_ref[...], wb_ref[...]], axis=0)
    for r in range(n_loc):
        if r in begins:
            m_copies[begins.index(r)].wait()
        value = m_ref[r].astype(F32)
        mean = jnp.sum(value, axis=0, keepdims=True) * (1.0 / msa_dim)
        centred = value - mean
        var = jnp.sum(centred * centred, axis=0, keepdims=True) * (1.0 / msa_dim)
        normed = centred * lax.rsqrt(var + LN_EPS)
        normed = (normed * scale + offset).astype(BF16)
        both = jnp.dot(w_ab, normed, preferred_element_type=F32) + bias
        for c in range(0, hid, 8):
            for t in range(n_seq // lanes):
                a_rows[t, pl.ds(c * n_loc + r, 8, stride=n_loc), :] = both[c:c + 8, t * lanes:(t + 1) * lanes]
        held[r * hid:(r + 1) * hid, :] = both[hid:].astype(BF16)
        if r in ends:
            if r == ends[0]:
                pl.semaphore_wait(barrier, len(peers))
            pass_on(OWN, ends.index(r), None)
    for t in range(n_seq // lanes):
        a_cols[t * lanes:(t + 1) * lanes, :] = a_rows[t].astype(BF16).T
    pass_on(OWN, len(ends) - 1, None)

    for copy in wo_copies:
        copy.wait()
    z_copy.wait()

    starts = [device(along, across, core if kind == "mine" else 1 - core) * n_loc for kind, along, across in units]
    actions = []
    for name, events in zip(units, before):
        todo = [functools.partial(receive, *event) for event in events]
        if name in block_index:
            todo.append(functools.partial(receive_block, name))
        actions.append(todo)

    inv_seq = 1.0 / n_seq
    bias_out = bo_ref[...].astype(F32)

    def step(index, carry):
        dispatch(index, 0, len(units), actions)
        start = starts[0]
        for k in range(1, len(units)):
            start = jnp.where(index == k, starts[k], start)
        here = pl.ds(pl.multiple_of(index * rows, rows), rows)
        for c in range(0, rows, 2 * lanes):
            prod = jnp.dot(held[here, :], a_cols[:, c:c + 2 * lanes], preferred_element_type=F32)
            outer[:, c:c + 2 * lanes] = (prod * inv_seq).astype(BF16)
        for j in range(n_loc):
            tile = jnp.concatenate([outer[j * hid:(j + 1) * hid, t * lanes:(t + 1) * lanes] for t in range(n_hi)], axis=0)
            turned = tile.T
            for k in range(n_lo):
                lhs[j * n_loc:(j + 1) * n_loc, k * lanes:(k + 1) * lanes] = turned[k * n_loc:(k + 1) * n_loc]
        w_all = wo_ref[...].reshape(n_lo * n_hi * hid, wo_ref.shape[-1])
        update = jnp.dot(lhs[...], w_all, preferred_element_type=F32) + bias_out
        for j in range(n_loc):
            for i in range(0, n_loc, 8):
                upd[pl.ds(i * n_loc + j, 8, stride=n_loc), :] = update[j * n_loc + i:j * n_loc + i + 8]
        cols = pl.ds(pl.multiple_of(start, n_loc), n_loc)
        total = z_ref[:, cols, :].astype(F32) + upd[...].reshape(n_loc, n_loc, upd.shape[-1])
        out_ref[:, cols, :] = total.astype(BF16)
        return carry

    lax.fori_loop(0, len(units), step, 0)

    for direction in peers:
        landed(held.at[pl.ds(0, sent[direction])], send_sem.at[lane_of[direction]])


def solution(mesh):
    row_spec = P(('batch', 'dap'))
    col_spec = P(None, ('batch', 'dap'))
    rep_spec = P()
    side = math.isqrt(mesh.shape['dap'] // CORES)
    units, before = plan(side)

    def local_update(z_rows, msa, ln_scale, ln_offset, w_a, b_a, w_b, b_b, w_out, b_out):
        n_seq, n_loc, msa_dim = msa.shape
        hid = w_a.shape[1]
        rows = n_loc * hid
        pair_dim = z_rows.shape[2]
        n_hi = rows // 128
        n_lo = hid // n_hi
        n_events = sum(len(events) for events in before)
        n_blocks = len(units) - 1 - n_events // len(PART_SIZES)
        row = lambda v: v.reshape(1, -1)
        any_spec = pl.BlockSpec(memory_space=pl.ANY)
        vmem_spec = pl.BlockSpec(memory_space=pltpu.VMEM)
        call = pl.pallas_call(
            functools.partial(kernel, side, units, before),
            out_shape=pltpu.VMEM(z_rows.shape, z_rows.dtype),
            in_specs=[any_spec] * 10,
            out_specs=vmem_spec,
            scratch_shapes=[
                pltpu.VMEM((n_loc, msa_dim, n_seq), BF16),
                pltpu.VMEM((1, msa_dim), BF16),
                pltpu.VMEM((1, msa_dim), BF16),
                pltpu.VMEM((hid, msa_dim), BF16),
                pltpu.VMEM((1, hid), BF16),
                pltpu.VMEM((hid, msa_dim), BF16),
                pltpu.VMEM((1, hid), BF16),
                pltpu.VMEM((n_lo, n_hi, hid, pair_dim), BF16),
                pltpu.VMEM((1, pair_dim), BF16),
                pltpu.VMEM(z_rows.shape, BF16),
                pltpu.VMEM((len(units) * rows, n_seq), BF16),
                pltpu.VMEM((n_seq // 128, rows, 128), F32),
                pltpu.VMEM((n_seq, rows), BF16),
                pltpu.VMEM((rows, rows), BF16),
                pltpu.VMEM((n_loc * n_loc, hid * hid), BF16),
                pltpu.VMEM((n_loc * n_loc, pair_dim), F32),
                pltpu.SemaphoreType.DMA((7,)),
                pltpu.SemaphoreType.DMA((len(PART_SIZES),)),
                pltpu.SemaphoreType.DMA((n_lo,)),
                pltpu.SemaphoreType.DMA,
                pltpu.SemaphoreType.DMA((3,)),
                pltpu.SemaphoreType.DMA((n_events,)),
                pltpu.SemaphoreType.DMA((n_blocks,)),
            ],
            compiler_params=pltpu.CompilerParams(
                collective_id=0, has_side_effects=True, vmem_limit_bytes=56 * 1024 * 1024),
            name="outer_product_mean",
        )
        return call(z_rows, msa.transpose(1, 2, 0), row(ln_scale), row(ln_offset), w_a.T, row(b_a), w_b.T, row(b_b),
                    w_out.reshape(n_hi, n_lo, hid, pair_dim), row(b_out))

    return jax.shard_map(local_update, mesh=mesh, in_specs=(row_spec, col_spec) + (rep_spec,) * 8, out_specs=row_spec, check_vma=False)
```

```python
import functools
import heapq
import itertools
import math

import jax
import jax.numpy as jnp
from jax import lax
from jax.experimental import pallas as pl
from jax.experimental.pallas import tpu as pltpu
from jax.sharding import PartitionSpec as P

LN_EPS = 1e-5
CORES = 2
HALVES = 2
FIRST_PIECE = 2
LINK_LATENCY = 5.0
PARTNER_LATENCY = 3.7
UNIT_TIME = 1.0
NORM_TIME = 0.26
MESH = pl.DeviceIdType.MESH
F32 = jnp.float32
BF16 = jnp.bfloat16
OWN = ("mine", 0, 0)


def forwards(name, half, over_link, side):
    kind, along, across = name
    hops = []
    if not over_link and along == 0 and (kind == "other" or across == 0):
        hops.append(("+", (kind, side - 1, across)))
        hops.append(("-", (kind, 1, across)))
    elif over_link and along == side - 1 and half == 0:
        hops.append(("+", (kind, along - 1, across)))
    elif over_link and along == 1 and half == 1:
        hops.append(("-", (kind, along + 1, across)))
    if over_link or name == OWN:
        hops.append(("core", ("other" if kind == "mine" else "mine", across, along)))
    return hops


def plan(side, n_loc):
    tick = itertools.count()
    size = n_loc // HALVES
    heap, free, events, ready = [], {"+": 0.0, "-": 0.0}, [], {}
    begin = NORM_TIME * n_loc + 1.5
    for half in range(HALVES):
        heapq.heappush(heap, (NORM_TIME * (half * size + FIRST_PIECE), next(tick), OWN, half, None))
        ready[OWN, half] = begin
    while heap:
        time, _, name, half, over_link = heapq.heappop(heap)
        if over_link is not None:
            ready[name, half] = time
            events.append((time, name, half, over_link))
        for direction, there in forwards(name, half, over_link, side):
            if direction == "core":
                at = time + PARTNER_LATENCY
            else:
                free[direction] = max(free[direction], time) + size
                at = free[direction] + LINK_LATENCY
            heapq.heappush(heap, (at, next(tick), there, half, direction != "core"))
    todo = sorted((time, name) for name, time in ready.items())
    units, before, waiting, now = [], [], [], begin
    while todo:
        if events and events[0][0] <= now:
            waiting.append(events.pop(0)[1:])
        elif todo[0][0] <= now:
            units.append(todo.pop(0)[1])
            before.append(waiting)
            waiting = []
            now += UNIT_TIME
        else:
            now = min([todo[0][0]] + [event[0] for event in events[:1]])
    return units, before


def column(row, size):
    shape = (size, size)
    eye = lax.broadcasted_iota(jnp.int32, shape, 0) == lax.broadcasted_iota(jnp.int32, shape, 1)
    return jnp.sum(jnp.where(eye, jnp.broadcast_to(row, shape), 0.0), axis=1, keepdims=True)


def dispatch(index, low, high, actions):
    if not any(actions[low:high]):
        return
    if high - low == 1:
        for action in actions[low]:
            action()
        return
    mid = (low + high) // 2
    if any(actions[low:mid]):
        pl.when(index < mid)(lambda: dispatch(index, low, mid, actions))
    if any(actions[mid:high]):
        pl.when(index >= mid)(lambda: dispatch(index, mid, high, actions))


def kernel(side, units, before, z_hbm, m_hbm, scale_hbm, offset_hbm, wa_hbm, ba_hbm, wb_hbm, bb_hbm, wo_hbm, bo_hbm, out_ref,
           m_ref, scale_ref, offset_ref, wa_ref, ba_ref, wb_ref, bb_ref, wo_ref, bo_ref, z_ref,
           held, a_rows, a_cols, outer, lhs, upd, in_sem, m_sem, wo_sem, z_sem, send_sem, recv_sem):
    n_loc, msa_dim, n_seq = m_ref.shape
    hid = wa_ref.shape[0]
    rows = n_loc * hid
    size = n_loc // HALVES
    part_rows = size * hid
    begins = [0, FIRST_PIECE] + [half * size for half in range(1, HALVES)]
    ends = begins[1:] + [n_loc]
    lanes = 128
    n_hi = rows // lanes
    n_lo = hid // n_hi

    me = lax.axis_index("dap")
    core = lax.rem(me, CORES)
    chip = me // CORES
    x, y = lax.rem(chip, side), chip // side
    pos_a = x * (1 - core) + y * core
    pos_b = y * (1 - core) + x * core

    def device(along, across, which):
        a, b = lax.rem(pos_a + along, side), lax.rem(pos_b + across, side)
        return ((b * (1 - core) + a * core) * side + a * (1 - core) + b * core) * CORES + which

    peers = {"+": device(1, 0, core), "-": device(side - 1, 0, core), "core": device(0, 0, 1 - core)}
    lane_of = {d: k for k, d in enumerate(peers)}
    slot = {name: k for k, name in enumerate(units)}
    barrier = pltpu.get_barrier_semaphore()
    for peer in peers.values():
        pl.semaphore_signal(barrier, inc=1, device_id={"dap": peer}, device_id_type=MESH)

    m_copies = []
    for k, (lo, hi) in enumerate(zip(begins, ends)):
        m_copies.append(pltpu.make_async_copy(m_hbm.at[lo:hi], m_ref.at[lo:hi], m_sem.at[k]))
    small = [pltpu.make_async_copy(s, d, in_sem.at[k]) for k, (s, d) in enumerate((
        (scale_hbm, scale_ref), (offset_hbm, offset_ref), (wa_hbm, wa_ref), (ba_hbm, ba_ref), (wb_hbm, wb_ref),
        (bb_hbm, bb_ref), (bo_hbm, bo_ref)))]
    wo_copies = [pltpu.make_async_copy(wo_hbm.at[:, k], wo_ref.at[k], wo_sem.at[k]) for k in range(n_lo)]
    z_copy = pltpu.make_async_copy(z_hbm, z_ref, z_sem)
    for copy in m_copies[:1] + small + m_copies[1:] + wo_copies + [z_copy]:
        copy.start()

    sent = {d: 0 for d in peers}

    def pass_on(name, half, over_link, lo=0, hi=size):
        for direction, there in forwards(name, half, over_link, side):
            sent[direction] += (hi - lo) * hid
            pltpu.make_async_remote_copy(
                src_ref=held.at[pl.ds(slot[name, half] * part_rows + lo * hid, (hi - lo) * hid)],
                dst_ref=held.at[pl.ds(slot[there, half] * part_rows + lo * hid, (hi - lo) * hid)],
                send_sem=send_sem.at[lane_of[direction]],
                recv_sem=recv_sem.at[slot[there, half]],
                device_id={"dap": peers[direction]},
                device_id_type=MESH,
            ).start()

    def landed(ref, sem):
        pltpu.make_async_copy(ref, ref, sem).wait()

    def receive(name, half, over_link):
        index = slot[name, half]
        landed(held.at[pl.ds(index * part_rows, part_rows)], recv_sem.at[index])
        pass_on(name, half, over_link)

    def send_own(piece):
        half = begins[piece] // size
        pass_on(OWN, half, None, begins[piece] - half * size, ends[piece] - half * size)

    for copy in small:
        copy.wait()
    scale = column(scale_ref[...].astype(F32), msa_dim)
    offset = column(offset_ref[...].astype(F32), msa_dim)
    bias = jnp.concatenate([column(ba_ref[...].astype(F32), hid), column(bb_ref[...].astype(F32), hid)], axis=0)
    w_ab = jnp.concatenate([wa_ref[...], wb_ref[...]], axis=0)
    for r in range(n_loc):
        if r in begins:
            m_copies[begins.index(r)].wait()
        value = m_ref[r].astype(F32)
        mean = jnp.sum(value, axis=0, keepdims=True) * (1.0 / msa_dim)
        centred = value - mean
        var = jnp.sum(centred * centred, axis=0, keepdims=True) * (1.0 / msa_dim)
        normed = centred * lax.rsqrt(var + LN_EPS)
        normed = (normed * scale + offset).astype(BF16)
        both = jnp.dot(w_ab, normed, preferred_element_type=F32) + bias
        for c in range(0, hid, 8):
            for t in range(n_seq // lanes):
                a_rows[t, pl.ds(c * n_loc + r, 8, stride=n_loc), :] = both[c:c + 8, t * lanes:(t + 1) * lanes]
        row = slot[OWN, r // size] * part_rows + r % size * hid
        held[row:row + hid, :] = both[hid:].astype(BF16)
        if r in ends:
            if r == ends[0]:
                pl.semaphore_wait(barrier, len(peers))
            send_own(ends.index(r))
    for t in range(n_seq // lanes):
        a_cols[t * lanes:(t + 1) * lanes, :] = a_rows[t].astype(BF16).T
    send_own(len(ends) - 1)

    for copy in wo_copies:
        copy.wait()
    z_copy.wait()

    starts = [device(along, across, core if kind == "mine" else 1 - core) * n_loc + half * size
              for (kind, along, across), half in units]
    actions = [[functools.partial(receive, *event) for event in events] for events in before]

    inv_seq = 1.0 / n_seq
    bias_out = bo_ref[...].astype(F32)

    def step(index, carry):
        dispatch(index, 0, len(units), actions)
        start = starts[0]
        for k in range(1, len(units)):
            start = jnp.where(index == k, starts[k], start)
        here = pl.ds(pl.multiple_of(index * part_rows, part_rows), part_rows)
        for c in range(0, rows, 2 * lanes):
            prod = jnp.dot(held[here, :], a_cols[:, c:c + 2 * lanes], preferred_element_type=F32)
            outer[:, c:c + 2 * lanes] = (prod * inv_seq).astype(BF16)
        for j in range(size):
            tile = jnp.concatenate([outer[j * hid:(j + 1) * hid, t * lanes:(t + 1) * lanes] for t in range(n_hi)], axis=0)
            turned = tile.T
            for k in range(n_lo):
                lhs[j * n_loc:(j + 1) * n_loc, k * lanes:(k + 1) * lanes] = turned[k * n_loc:(k + 1) * n_loc]
        w_all = wo_ref[...].reshape(n_lo * n_hi * hid, wo_ref.shape[-1])
        update = jnp.dot(lhs[...], w_all, preferred_element_type=F32) + bias_out
        for j in range(size):
            for i in range(0, n_loc, 8):
                upd[pl.ds(i * size + j, 8, stride=size), :] = update[j * n_loc + i:j * n_loc + i + 8]
        cols = pl.ds(pl.multiple_of(start, size), size)
        total = z_ref[:, cols, :].astype(F32) + upd[...].reshape(n_loc, size, upd.shape[-1])
        out_ref[:, cols, :] = total.astype(BF16)
        return carry

    lax.fori_loop(0, len(units), step, 0)

    for direction in peers:
        landed(held.at[pl.ds(0, sent[direction])], send_sem.at[lane_of[direction]])


def solution(mesh):
    row_spec = P(('batch', 'dap'))
    col_spec = P(None, ('batch', 'dap'))
    rep_spec = P()
    side = math.isqrt(mesh.shape['dap'] // CORES)
    def local_update(z_rows, msa, ln_scale, ln_offset, w_a, b_a, w_b, b_b, w_out, b_out):
        n_seq, n_loc, msa_dim = msa.shape
        hid = w_a.shape[1]
        rows = n_loc * hid
        pair_dim = z_rows.shape[2]
        n_hi = rows // 128
        n_lo = hid // n_hi
        units, before = plan(side, n_loc)
        row = lambda v: v.reshape(1, -1)
        any_spec = pl.BlockSpec(memory_space=pl.ANY)
        vmem_spec = pl.BlockSpec(memory_space=pltpu.VMEM)
        call = pl.pallas_call(
            functools.partial(kernel, side, units, before),
            out_shape=pltpu.VMEM(z_rows.shape, z_rows.dtype),
            in_specs=[any_spec] * 10,
            out_specs=vmem_spec,
            scratch_shapes=[
                pltpu.VMEM((n_loc, msa_dim, n_seq), BF16),
                pltpu.VMEM((1, msa_dim), BF16),
                pltpu.VMEM((1, msa_dim), BF16),
                pltpu.VMEM((hid, msa_dim), BF16),
                pltpu.VMEM((1, hid), BF16),
                pltpu.VMEM((hid, msa_dim), BF16),
                pltpu.VMEM((1, hid), BF16),
                pltpu.VMEM((n_lo, n_hi, hid, pair_dim), BF16),
                pltpu.VMEM((1, pair_dim), BF16),
                pltpu.VMEM(z_rows.shape, BF16),
                pltpu.VMEM((len(units) * rows // HALVES, n_seq), BF16),
                pltpu.VMEM((n_seq // 128, rows, 128), F32),
                pltpu.VMEM((n_seq, rows), BF16),
                pltpu.VMEM((rows // HALVES, rows), BF16),
                pltpu.VMEM((n_loc * n_loc // HALVES, hid * hid), BF16),
                pltpu.VMEM((n_loc * n_loc // HALVES, pair_dim), F32),
                pltpu.SemaphoreType.DMA((7,)),
                pltpu.SemaphoreType.DMA((HALVES + 1,)),
                pltpu.SemaphoreType.DMA((n_lo,)),
                pltpu.SemaphoreType.DMA,
                pltpu.SemaphoreType.DMA((3,)),
                pltpu.SemaphoreType.DMA((len(units),)),
            ],
            compiler_params=pltpu.CompilerParams(
                collective_id=0, has_side_effects=True, vmem_limit_bytes=56 * 1024 * 1024),
            name="outer_product_mean",
        )
        return call(z_rows, msa.transpose(1, 2, 0), row(ln_scale), row(ln_offset), w_a.T, row(b_a), w_b.T, row(b_b),
                    w_out.reshape(n_hi, n_lo, hid, pair_dim), row(b_out))

    return jax.shard_map(local_update, mesh=mesh, in_specs=(row_spec, col_spec) + (rep_spec,) * 8, out_specs=row_spec, check_vma=False)
```

```python
import functools
import heapq
import itertools
import math

import jax
import jax.numpy as jnp
from jax import lax
from jax.experimental import pallas as pl
from jax.experimental.pallas import tpu as pltpu
from jax.sharding import PartitionSpec as P

LN_EPS = 1e-5
CORES = 2
HALVES = 2
FIRST_PIECE = 2
LINK_LATENCY = 5.0
PARTNER_LATENCY = 5.0
PARTNER_TIME = 0.3
UNIT_TIME = 1.1
NORM_TIME = 0.26
MESH = pl.DeviceIdType.MESH
F32 = jnp.float32
BF16 = jnp.bfloat16
OWN = ("mine", 0, 0)


def forwards(name, half, over_link, side):
    kind, along, across = name
    hops = []
    if not over_link and along == 0 and (kind == "other" or across == 0):
        hops.append(("+", (kind, side - 1, across)))
        hops.append(("-", (kind, 1, across)))
    elif over_link and along == side - 1 and half == 0:
        hops.append(("+", (kind, along - 1, across)))
    elif over_link and along == 1 and half == 1:
        hops.append(("-", (kind, along + 1, across)))
    if over_link or name == OWN:
        hops.append(("core", ("other" if kind == "mine" else "mine", across, along)))
    return hops


def plan(side, n_loc):
    tick = itertools.count()
    size = n_loc // HALVES
    heap, free, events, ready = [], {"+": 0.0, "-": 0.0, "core": 0.0}, [], {}
    begin = NORM_TIME * n_loc + 1.5
    for half in range(HALVES):
        heapq.heappush(heap, (NORM_TIME * (half * size + FIRST_PIECE), next(tick), OWN, half, None))
        ready[OWN, half] = begin
    while heap:
        time, _, name, half, over_link = heapq.heappop(heap)
        if over_link is not None:
            ready[name, half] = time
            events.append((time, name, half, over_link))
        for direction, there in forwards(name, half, over_link, side):
            busy, latency = (PARTNER_TIME, PARTNER_LATENCY) if direction == "core" else (1.0, LINK_LATENCY)
            free[direction] = max(free[direction], time) + busy * size
            at = free[direction] + latency
            heapq.heappush(heap, (at, next(tick), there, half, direction != "core"))
    todo = sorted((time, name) for name, time in ready.items())
    units, before, waiting, now = [], [], [], begin
    while todo:
        if events and events[0][0] <= now:
            waiting.append(events.pop(0)[1:])
        elif todo[0][0] <= now:
            units.append(todo.pop(0)[1])
            before.append(waiting)
            waiting = []
            now += UNIT_TIME
        else:
            now = min([todo[0][0]] + [event[0] for event in events[:1]])
    return units, before


def column(row, size):
    shape = (size, size)
    eye = lax.broadcasted_iota(jnp.int32, shape, 0) == lax.broadcasted_iota(jnp.int32, shape, 1)
    return jnp.sum(jnp.where(eye, jnp.broadcast_to(row, shape), 0.0), axis=1, keepdims=True)


def dispatch(index, low, high, actions):
    if not any(actions[low:high]):
        return
    if high - low == 1:
        for action in actions[low]:
            action()
        return
    mid = (low + high) // 2
    if any(actions[low:mid]):
        pl.when(index < mid)(lambda: dispatch(index, low, mid, actions))
    if any(actions[mid:high]):
        pl.when(index >= mid)(lambda: dispatch(index, mid, high, actions))


def kernel(side, units, before, z_hbm, m_hbm, scale_hbm, offset_hbm, wa_hbm, ba_hbm, wb_hbm, bb_hbm, wo_hbm, bo_hbm, out_ref,
           m_ref, scale_ref, offset_ref, wa_ref, ba_ref, wb_ref, bb_ref, wo_ref, bo_ref, z_ref,
           held, a_rows, a_cols, outer, lhs, upd, in_sem, m_sem, wo_sem, z_sem, send_sem, recv_sem):
    n_loc, msa_dim, n_seq = m_ref.shape
    hid = wa_ref.shape[0]
    rows = n_loc * hid
    size = n_loc // HALVES
    part_rows = size * hid
    begins = [0, FIRST_PIECE] + [half * size for half in range(1, HALVES)]
    ends = begins[1:] + [n_loc]
    lanes = 128
    n_hi = rows // lanes
    n_lo = hid // n_hi

    me = lax.axis_index("dap")
    core = lax.rem(me, CORES)
    chip = me // CORES
    x, y = lax.rem(chip, side), chip // side
    pos_a = x * (1 - core) + y * core
    pos_b = y * (1 - core) + x * core

    def device(along, across, which):
        a, b = lax.rem(pos_a + along, side), lax.rem(pos_b + across, side)
        return ((b * (1 - core) + a * core) * side + a * (1 - core) + b * core) * CORES + which

    peers = {"+": device(1, 0, core), "-": device(side - 1, 0, core), "core": device(0, 0, 1 - core)}
    lane_of = {d: k for k, d in enumerate(peers)}
    slot = {name: k for k, name in enumerate(units)}
    barrier = pltpu.get_barrier_semaphore()
    for peer in peers.values():
        pl.semaphore_signal(barrier, inc=1, device_id={"dap": peer}, device_id_type=MESH)

    m_copies = []
    for k, (lo, hi) in enumerate(zip(begins, ends)):
        m_copies.append(pltpu.make_async_copy(m_hbm.at[lo:hi], m_ref.at[lo:hi], m_sem.at[k]))
    small = [pltpu.make_async_copy(s, d, in_sem.at[k]) for k, (s, d) in enumerate((
        (scale_hbm, scale_ref), (offset_hbm, offset_ref), (wa_hbm, wa_ref), (ba_hbm, ba_ref), (wb_hbm, wb_ref),
        (bb_hbm, bb_ref), (bo_hbm, bo_ref)))]
    wo_copies = [pltpu.make_async_copy(wo_hbm.at[:, k], wo_ref.at[k], wo_sem.at[k]) for k in range(n_lo)]
    z_copy = pltpu.make_async_copy(z_hbm, z_ref, z_sem)
    for copy in m_copies[:1] + small + m_copies[1:] + wo_copies + [z_copy]:
        copy.start()

    sent = {d: 0 for d in peers}

    def pass_on(name, half, over_link, lo=0, hi=size):
        for direction, there in forwards(name, half, over_link, side):
            sent[direction] += (hi - lo) * hid
            pltpu.make_async_remote_copy(
                src_ref=held.at[pl.ds(slot[name, half] * part_rows + lo * hid, (hi - lo) * hid)],
                dst_ref=held.at[pl.ds(slot[there, half] * part_rows + lo * hid, (hi - lo) * hid)],
                send_sem=send_sem.at[lane_of[direction]],
                recv_sem=recv_sem.at[slot[there, half]],
                device_id={"dap": peers[direction]},
                device_id_type=MESH,
            ).start()

    def landed(ref, sem):
        pltpu.make_async_copy(ref, ref, sem).wait()

    def receive(name, half, over_link):
        index = slot[name, half]
        landed(held.at[pl.ds(index * part_rows, part_rows)], recv_sem.at[index])
        pass_on(name, half, over_link)

    def send_own(piece):
        half = begins[piece] // size
        pass_on(OWN, half, None, begins[piece] - half * size, ends[piece] - half * size)

    for copy in small:
        copy.wait()
    scale = column(scale_ref[...].astype(F32), msa_dim)
    offset = column(offset_ref[...].astype(F32), msa_dim)
    bias = jnp.concatenate([column(ba_ref[...].astype(F32), hid), column(bb_ref[...].astype(F32), hid)], axis=0)
    w_ab = jnp.concatenate([wa_ref[...], wb_ref[...]], axis=0)
    for r in range(n_loc):
        if r in begins:
            m_copies[begins.index(r)].wait()
        value = m_ref[r].astype(F32)
        mean = jnp.sum(value, axis=0, keepdims=True) * (1.0 / msa_dim)
        centred = value - mean
        var = jnp.sum(centred * centred, axis=0, keepdims=True) * (1.0 / msa_dim)
        normed = centred * lax.rsqrt(var + LN_EPS)
        normed = (normed * scale + offset).astype(BF16)
        both = jnp.dot(w_ab, normed, preferred_element_type=F32) + bias
        for c in range(0, hid, 8):
            for t in range(n_seq // lanes):
                a_rows[t, pl.ds(c * n_loc + r, 8, stride=n_loc), :] = both[c:c + 8, t * lanes:(t + 1) * lanes]
        row = slot[OWN, r // size] * part_rows + r % size * hid
        held[row:row + hid, :] = both[hid:].astype(BF16)
        if r in ends:
            if r == ends[0]:
                pl.semaphore_wait(barrier, len(peers))
            send_own(ends.index(r))
    for t in range(n_seq // lanes):
        a_cols[t * lanes:(t + 1) * lanes, :] = a_rows[t].astype(BF16).T
    send_own(len(ends) - 1)

    for copy in wo_copies:
        copy.wait()
    z_copy.wait()

    starts = [device(along, across, core if kind == "mine" else 1 - core) * n_loc + half * size
              for (kind, along, across), half in units]
    actions = [[functools.partial(receive, *event) for event in events] for events in before]

    inv_seq = 1.0 / n_seq
    bias_out = bo_ref[...].astype(F32)

    def step(index, carry):
        dispatch(index, 0, len(units), actions)
        start = starts[0]
        for k in range(1, len(units)):
            start = jnp.where(index == k, starts[k], start)
        here = pl.ds(pl.multiple_of(index * part_rows, part_rows), part_rows)
        for c in range(0, rows, 2 * lanes):
            prod = jnp.dot(held[here, :], a_cols[:, c:c + 2 * lanes], preferred_element_type=F32)
            outer[:, c:c + 2 * lanes] = (prod * inv_seq).astype(BF16)
        for j in range(size):
            tile = jnp.concatenate([outer[j * hid:(j + 1) * hid, t * lanes:(t + 1) * lanes] for t in range(n_hi)], axis=0)
            turned = tile.T
            for k in range(n_lo):
                lhs[j * n_loc:(j + 1) * n_loc, k * lanes:(k + 1) * lanes] = turned[k * n_loc:(k + 1) * n_loc]
        w_all = wo_ref[...].reshape(n_lo * n_hi * hid, wo_ref.shape[-1])
        update = jnp.dot(lhs[...], w_all, preferred_element_type=F32) + bias_out
        for j in range(size):
            for i in range(0, n_loc, 8):
                upd[pl.ds(i * size + j, 8, stride=size), :] = update[j * n_loc + i:j * n_loc + i + 8]
        cols = pl.ds(pl.multiple_of(start, size), size)
        total = z_ref[:, cols, :].astype(F32) + upd[...].reshape(n_loc, size, upd.shape[-1])
        out_ref[:, cols, :] = total.astype(BF16)
        return carry

    lax.fori_loop(0, len(units), step, 0)

    for direction in peers:
        landed(held.at[pl.ds(0, sent[direction])], send_sem.at[lane_of[direction]])


def solution(mesh):
    row_spec = P(('batch', 'dap'))
    col_spec = P(None, ('batch', 'dap'))
    rep_spec = P()
    side = math.isqrt(mesh.shape['dap'] // CORES)
    def local_update(z_rows, msa, ln_scale, ln_offset, w_a, b_a, w_b, b_b, w_out, b_out):
        n_seq, n_loc, msa_dim = msa.shape
        hid = w_a.shape[1]
        rows = n_loc * hid
        pair_dim = z_rows.shape[2]
        n_hi = rows // 128
        n_lo = hid // n_hi
        units, before = plan(side, n_loc)
        row = lambda v: v.reshape(1, -1)
        any_spec = pl.BlockSpec(memory_space=pl.ANY)
        vmem_spec = pl.BlockSpec(memory_space=pltpu.VMEM)
        call = pl.pallas_call(
            functools.partial(kernel, side, units, before),
            out_shape=pltpu.VMEM(z_rows.shape, z_rows.dtype),
            in_specs=[any_spec] * 10,
            out_specs=vmem_spec,
            scratch_shapes=[
                pltpu.VMEM((n_loc, msa_dim, n_seq), BF16),
                pltpu.VMEM((1, msa_dim), BF16),
                pltpu.VMEM((1, msa_dim), BF16),
                pltpu.VMEM((hid, msa_dim), BF16),
                pltpu.VMEM((1, hid), BF16),
                pltpu.VMEM((hid, msa_dim), BF16),
                pltpu.VMEM((1, hid), BF16),
                pltpu.VMEM((n_lo, n_hi, hid, pair_dim), BF16),
                pltpu.VMEM((1, pair_dim), BF16),
                pltpu.VMEM(z_rows.shape, BF16),
                pltpu.VMEM((len(units) * rows // HALVES, n_seq), BF16),
                pltpu.VMEM((n_seq // 128, rows, 128), F32),
                pltpu.VMEM((n_seq, rows), BF16),
                pltpu.VMEM((rows // HALVES, rows), BF16),
                pltpu.VMEM((n_loc * n_loc // HALVES, hid * hid), BF16),
                pltpu.VMEM((n_loc * n_loc // HALVES, pair_dim), F32),
                pltpu.SemaphoreType.DMA((7,)),
                pltpu.SemaphoreType.DMA((HALVES + 1,)),
                pltpu.SemaphoreType.DMA((n_lo,)),
                pltpu.SemaphoreType.DMA,
                pltpu.SemaphoreType.DMA((3,)),
                pltpu.SemaphoreType.DMA((len(units),)),
            ],
            compiler_params=pltpu.CompilerParams(
                collective_id=0, has_side_effects=True, vmem_limit_bytes=56 * 1024 * 1024),
            name="outer_product_mean",
        )
        return call(z_rows, msa.transpose(1, 2, 0), row(ln_scale), row(ln_offset), w_a.T, row(b_a), w_b.T, row(b_b),
                    w_out.reshape(n_hi, n_lo, hid, pair_dim), row(b_out))

    return jax.shard_map(local_update, mesh=mesh, in_specs=(row_spec, col_spec) + (rep_spec,) * 8, out_specs=row_spec, check_vma=False)
```
